8 devices in a mesh: rep: 2 (over y, z), dp: 4 (over x, core).
Axes of the slice: x: 2, y: 2, z: 1, core: 2. Of those that a mesh axis runs over, the one named last changes fastest.
Arguments:
- g_w_gate: bfloat16 [8, 2, 1152, 4608], P(('rep', 'dp')), parts along dimension 0
- g_w_up: bfloat16 [8, 2, 1152, 4608], P(('rep', 'dp')), parts along dimension 0
- g_w_down: bfloat16 [8, 2, 4608, 1152], P(('rep', 'dp')), parts along dimension 0
- w_gate: bfloat16 [2, 1152, 4608], replicated
- w_up: bfloat16 [2, 1152, 4608], replicated
- w_down: bfloat16 [2, 4608, 1152], replicated
- m_w_gate: float32 [2, 1152, 4608], P(None, 'dp')
- m_w_up: float32 [2, 1152, 4608], P(None, 'dp')
- m_w_down: float32 [2, 4608, 1152], P(None, 'dp')
- v_w_gate: float32 [2, 1152, 4608], P(None, 'dp')
- v_w_up: float32 [2, 1152, 4608], P(None, 'dp')
- v_w_down: float32 [2, 4608, 1152], P(None, 'dp')
Outputs:
- output 1: bfloat16 [4, 1152, 4608], P('rep'), parts along dimension 0
- output 2: bfloat16 [4, 1152, 4608], P('rep'), parts along dimension 0
- output 3: bfloat16 [4, 4608, 1152], P('rep'), parts along dimension 0
- output 4: float32 [4, 1152, 4608], P('rep', 'dp'), parts along dimension 0
- output 5: float32 [4, 1152, 4608], P('rep', 'dp'), parts along dimension 0
- output 6: float32 [4, 4608, 1152], P('rep', 'dp'), parts along dimension 0
- output 7: float32 [4, 1152, 4608], P('rep', 'dp'), parts along dimension 0
- output 8: float32 [4, 1152, 4608], P('rep', 'dp'), parts along dimension 0
- output 9: float32 [4, 4608, 1152], P('rep', 'dp'), parts along dimension 0
There are 2 independent parts. The reference program is written for one: setup_inputs(seed, part) draws one part's arguments, and reference() takes and returns one part's arrays. A program takes and returns all parts, laid end to end along the dimension named above; an argument that names none is the same for every part.
All inputs are finite; a program needn't handle non-finite values.
Results may differ from the reference program's by a relative error of at most 0.022.
Values are sent between devices in bfloat16 or wider.
A program may use at most 2 GiB of HBM per device.

```python
import jax
import jax.numpy as jnp
from jax import lax

DEVICES = 4
D = 1152
FF = 4608
LAYERS = 2
NAMES = ("w_gate", "w_up", "w_down")
SHAPES = {"w_gate": (LAYERS, D, FF), "w_up": (LAYERS, D, FF), "w_down": (LAYERS, FF, D)}


def setup_inputs(seed: int = 0, part: int = 0) -> dict:
    kz, *keys = jax.random.split(jax.random.key(seed), 1 + 5 * len(NAMES))
    loud = 2.0 ** jax.random.uniform(kz, (), jnp.float32, -1.0, 1.0)
    drawn = {}
    for name, key, both in zip(NAMES, keys[:3], keys[3:6], strict=True):
        own = jax.random.normal(jax.random.fold_in(key, part), (DEVICES, *SHAPES[name]), jnp.float32)
        shared = jax.random.normal(jax.random.fold_in(both, part), SHAPES[name], jnp.float32)
        drawn["g_" + name] = (loud * (0.7 * shared / DEVICES + 0.7 * own * DEVICES**-0.5)).astype(jnp.bfloat16)
    for name, key in zip(NAMES, keys[6:9], strict=True):
        drawn[name] = (jax.random.normal(key, SHAPES[name], jnp.float32) * SHAPES[name][1] ** -0.5).astype(jnp.bfloat16)
    for name, key in zip(NAMES, keys[9:12], strict=True):
        drawn["m_" + name] = loud * 0.5 * jax.random.normal(key, SHAPES[name], jnp.float32)
    for name, key in zip(NAMES, keys[12:15], strict=True):
        drawn["v_" + name] = loud * loud * jax.random.uniform(key, SHAPES[name], jnp.float32, 0.5, 1.5)
    return drawn


def adamw(w, m, v, g):
    m = 0.9 * m + 0.1 * g
    v = 0.95 * v + 0.05 * g * g
    step = m * lax.rsqrt(v + 1e-8) + 0.1 * w
    return (w - 0.02 * step).astype(jnp.bfloat16), m, v


def reference(g_w_gate, g_w_up, g_w_down, w_gate, w_up, w_down, m_w_gate, m_w_up, m_w_down, v_w_gate, v_w_up, v_w_down):
    def total(terms):
        return lax.scan(lambda so_far, term: (so_far + term.astype(jnp.float32), None), jnp.zeros(terms.shape[1:], jnp.float32), terms)[0]

    gradients = [total(terms).astype(jnp.bfloat16).astype(jnp.float32) for terms in (g_w_gate, g_w_up, g_w_down)]
    new = [
        adamw(w.astype(jnp.float32), m, v, g)
        for w, m, v, g in zip((w_gate, w_up, w_down), (m_w_gate, m_w_up, m_w_down), (v_w_gate, v_w_up, v_w_down), gradients, strict=True)
    ]
    return tuple(one[which] for which in range(3) for one in new)
```

```python
import jax
import jax.numpy as jnp
from jax import lax
from jax.experimental import pallas as pl
from jax.experimental.pallas import tpu as pltpu
from jax.sharding import PartitionSpec as P


MESH = pl.DeviceIdType.MESH
BF16, F32 = jnp.bfloat16, jnp.float32
ANY = pl.BlockSpec(memory_space=pl.ANY)
PER_LAYER = 6


PARTNER = [(i, i ^ 1) for i in range(4)]
ACROSS = [(i, i ^ 2) for i in range(4)]


def pair_sums(*refs):
    g = refs[0:3]
    across0 = refs[3]
    theirs = refs[4:7]
    sums = (None, *refs[7:9])
    mine, landed = refs[9:12], refs[12:15]
    in_send, in_recv, load, out_send, out_recv, store, own_send, own_recv = refs[15:]

    rep, me = lax.axis_index("rep"), lax.axis_index("dp")
    chip, core = me // 2, me % 2
    partner = chip * 2 + (1 - core)
    across = (1 - chip) * 2 + core
    diagonal = (1 - chip) * 2 + (1 - core)

    barrier = pltpu.get_barrier_semaphore()
    for other in (partner, across):
        pl.semaphore_signal(barrier, inc=1, device_id=(rep, other), device_id_type=MESH)
    pl.semaphore_wait(barrier, 2)

    def piece(w, owner, t):
        rows = mine[w].shape[1]
        return g[w].at[0, t // PER_LAYER, pl.ds((owner * PER_LAYER + t % PER_LAYER) * rows, rows)]

    def place(ref, w, t):
        rows = mine[w].shape[1]
        return ref.at[t // PER_LAYER, pl.ds((t % PER_LAYER) * rows, rows)]

    def to_partner(w, t):
        return pltpu.make_async_remote_copy(
            piece(w, diagonal, t), landed[w].at[t], in_send.at[w, t], in_recv.at[w, t], device_id=(rep, partner), device_id_type=MESH
        )

    def to_mine(w, t):
        return pltpu.make_async_copy(piece(w, across, t), mine[w].at[t], load.at[w, t])

    def send_across(t):
        return pltpu.make_async_remote_copy(
            mine[0].at[t], place(across0, 0, t), out_send.at[t], out_recv.at[t], device_id=(rep, across), device_id_type=MESH
        )

    def keep(w, t):
        return pltpu.make_async_copy(mine[w].at[t], place(sums[w], w, t), store.at[w - 1, t])

    def own_terms(w):
        rows = theirs[w].shape[1]
        return pltpu.make_async_remote_copy(
            g[w].at[0, :, pl.ds(partner * rows, rows)], theirs[w], own_send.at[w], own_recv.at[w], device_id=(rep, partner), device_id_type=MESH
        )

    def add(w, t):
        to_partner(w, t).wait_recv()
        to_mine(w, t).wait()
        mine[w][t] = (mine[w][t].astype(F32) + landed[w][t].astype(F32)).astype(BF16)

    pieces = 2 * PER_LAYER

    @pl.loop(0, pieces)
    def _(t):
        to_partner(0, t).start()
        to_mine(0, t).start()

    @pl.loop(0, pieces)
    def _(t):
        add(0, t)
        send_across(t).start()
        for w in (1, 2):
            to_partner(w, t).start()
            to_mine(w, t).start()

    for w in range(3):
        own_terms(w).start()

    for w in (1, 2):

        @pl.loop(0, pieces)
        def _(t, w=w):
            add(w, t)
            keep(w, t).start()

    @pl.loop(0, pieces)
    def _(t):
        for w in range(3):
            to_partner(w, t).wait_send()
        for w in (1, 2):
            keep(w, t).wait()

    for w in range(3):
        own_terms(w).wait()

    @pl.loop(0, pieces)
    def _(t):
        send_across(t).wait()


def exchange(terms, blocks):
    shapes = [(2, *b) for b in blocks]
    vmem = [pltpu.VMEM((2 * PER_LAYER, b[0] // PER_LAYER, b[1]), BF16) for b in blocks]
    pieces = 2 * PER_LAYER
    dma = pltpu.SemaphoreType.DMA
    return pl.pallas_call(
        pair_sums,
        out_shape=[jax.ShapeDtypeStruct(s, BF16) for s in (shapes[0], *shapes, *shapes[1:])],
        in_specs=[ANY] * 3,
        out_specs=[ANY] * 6,
        scratch_shapes=[
            *vmem,
            *vmem,
            dma((3, pieces)),
            dma((3, pieces)),
            dma((3, pieces)),
            dma((pieces,)),
            dma((pieces,)),
            dma((2, pieces)),
            dma((3,)),
            dma((3,)),
        ],
        compiler_params=pltpu.CompilerParams(collective_id=0, has_side_effects=True, vmem_limit_bytes=60 << 20),
        cost_estimate=pl.CostEstimate(flops=10**8, bytes_accessed=10**8, transcendentals=0),
        name="pair_sums",
    )(*terms)


def adamw(splits, where, g, theirs, arrived, m, v, w):
    layers, block, columns = m.shape
    rows = block // PER_LAYER
    steps = layers * PER_LAYER
    firsts = [first // rows for first, _ in splits]
    counts = [size // rows for _, size in splits]

    def body(where_ref, g_ref, theirs_ref, arrived_ref, m_ref, v_ref, w_ref, m_out, v_out, w_out, *parts):
        total = (g_ref[0, 0].astype(F32) + theirs_ref[0].astype(F32)) + arrived_ref[0].astype(F32)
        grad = total.astype(BF16).astype(F32)
        old = w_ref[0].astype(F32)
        new_m = 0.9 * m_ref[0] + 0.1 * grad
        new_v = 0.95 * v_ref[0] + 0.05 * grad * grad
        step = new_m * lax.rsqrt(new_v + 1e-8) + 0.1 * old
        new_w = (old - 0.02 * step).astype(BF16)
        m_out[0] = new_m
        v_out[0] = new_v
        w_out[0] = new_w
        i = pl.program_id(0)
        for part, first, count in zip(parts, firsts, counts, strict=True):

            @pl.when((i >= first) & (i < first + count))
            def _(part=part):
                part[...] = new_w

    def own(i, where):
        return (i // PER_LAYER, i % PER_LAYER, 0)

    def inside(i, where):
        return (i // PER_LAYER, where[0] * PER_LAYER + i % PER_LAYER, 0)

    def part_map(first, count):
        return lambda i, where: (jnp.clip(i - first, 0, count - 1), 0)

    tile = (1, rows, columns)
    return pl.pallas_call(
        body,
        grid_spec=pltpu.PrefetchScalarGridSpec(
            num_scalar_prefetch=1,
            grid=(steps,),
            in_specs=[
                pl.BlockSpec((1, *tile), lambda i, where: (0, *inside(i, where))),
                pl.BlockSpec(tile, own),
                pl.BlockSpec(tile, own),
                pl.BlockSpec(tile, own),
                pl.BlockSpec(tile, own),
                pl.BlockSpec(tile, inside),
            ],
            out_specs=[
                pl.BlockSpec(tile, own),
                pl.BlockSpec(tile, own),
                pl.BlockSpec(tile, inside),
                *(pl.BlockSpec((rows, columns), part_map(f, c)) for f, c in zip(firsts, counts, strict=True)),
            ],
        ),
        out_shape=[
            jax.ShapeDtypeStruct(m.shape, F32),
            jax.ShapeDtypeStruct(m.shape, F32),
            jax.ShapeDtypeStruct(w.shape, BF16),
            *(jax.ShapeDtypeStruct((size, columns), BF16) for _, size in splits),
        ],
        cost_estimate=pl.CostEstimate(flops=10**10, bytes_accessed=10**8, transcendentals=0),
        name="adamw",
    )(where, g, theirs, arrived, m, v, w)


def put(where, whole, after, block, first, arrived):
    columns = whole.shape[2]
    rows = block // PER_LAYER
    count = min(a.shape[0] for _, _, a in arrived) // rows
    n = len(arrived)

    def body(where_ref, *refs):
        out = refs[-1]
        j = pl.program_id(1)
        for k in range(n):

            @pl.when(j == k)
            def _(k=k):
                out[0] = refs[k][...]

    def in_map(skip):
        return lambda i, j, where: (i + skip // rows, 0)

    def out_map(i, j, where):
        t = i + first // rows
        owner = where[arrived[0][0]]
        for k in range(1, n):
            owner = jnp.where(j == k, where[arrived[k][0]], owner)
        return (t // PER_LAYER, owner * PER_LAYER + t % PER_LAYER, 0)

    return pl.pallas_call(
        body,
        grid_spec=pltpu.PrefetchScalarGridSpec(
            num_scalar_prefetch=1,
            grid=(count, n),
            in_specs=[*(pl.BlockSpec((rows, columns), in_map(skip)) for _, skip, _ in arrived), ANY, ANY],
            out_specs=pl.BlockSpec((1, rows, columns), out_map),
        ),
        out_shape=jax.ShapeDtypeStruct(whole.shape, BF16),
        input_output_aliases={n + 1: 0},
        compiler_params=pltpu.CompilerParams(vmem_limit_bytes=16 << 20),
        cost_estimate=pl.CostEstimate(flops=10**9, bytes_accessed=10**7, transcendentals=0),
        name="put",
    )(where, *(a for _, _, a in arrived), whole, after)


def send(array, pairs):
    return lax.ppermute(array, "dp", pairs)


def solution(mesh):
    def step(*arrays):
        terms, weights, ms, vs = (arrays[i : i + 3] for i in (0, 3, 6, 9))
        blocks = [m.shape[1:] for m in ms]
        where = lax.axis_index("dp") ^ jnp.arange(4, dtype=jnp.int32)
        across0, theirs0, theirs1, theirs2, sum1, sum2 = exchange(terms, blocks)
        arrived = [across0, send(sum1, ACROSS), send(sum2, ACROSS)]
        theirs = [theirs0, theirs1, theirs2]
        new_w, new_m, new_v = [], [], []
        after = where
        for k in range(3):
            block = blocks[k][0]
            rows = block // PER_LAYER
            splits = [(0, 2 * block)]
            if k == 2:
                sizes = (block, 4 * rows, rows, rows)
                splits += [(sum(sizes[:i]), sizes[i]) for i in range(4)]
            m, v, w, block_w, *parts = adamw(splits, where, terms[k], theirs[k], arrived[k], ms[k], vs[k], weights[k])
            parts = parts or [block_w]
            over = [send(a, ACROSS) for a in parts]
            beside = send(block_w, PARTNER)
            passed = [send(a, PARTNER) for a in over]
            first = 0
            for a, b in zip(over, passed, strict=True):
                w = put(where, w, after, block, first, [(1, first, beside), (2, 0, a), (3, 0, b)])
                first += a.shape[0]
            after = w
            new_w.append(w)
            new_m.append(m)
            new_v.append(v)
        return (*new_w, *new_m, *new_v)

    all_of, cut = P(None, None, None), P(None, "dp", None)
    return jax.shard_map(
        step,
        mesh=mesh,
        in_specs=(P(("rep", "dp"), None, None, None),) * 3 + (all_of,) * 3 + (cut,) * 6,
        out_specs=(P("rep", None, None),) * 3 + (P("rep", "dp", None),) * 6,
        check_vma=False,
    )
```

```python
import jax
import jax.numpy as jnp
from jax import lax
from jax.experimental import pallas as pl
from jax.experimental.pallas import tpu as pltpu
from jax.sharding import PartitionSpec as P


MESH = pl.DeviceIdType.MESH
BF16, F32 = jnp.bfloat16, jnp.float32
ANY = pl.BlockSpec(memory_space=pl.ANY)
HBM = pl.BlockSpec(memory_space=pltpu.HBM)
SUM_PIECES = (9, 6, 6)
STEP_PIECES = (6, 6, 12)
LATE = 12


PARTNER = [(i, i ^ 1) for i in range(4)]
ACROSS = [(i, i ^ 2) for i in range(4)]


def pair_sums(*refs):
    g = refs[0:3]
    across0 = refs[3]
    theirs = refs[4:7]
    sums = (None, *refs[7:9])
    mine, landed = refs[9:12], refs[12:15]
    in_send, in_recv, load = refs[15:18], refs[18:21], refs[21:24]
    out_send, out_recv, store, own_send, own_recv = refs[24:]

    rep, me = lax.axis_index("rep"), lax.axis_index("dp")
    chip, core = me // 2, me % 2
    partner = chip * 2 + (1 - core)
    across = (1 - chip) * 2 + core
    diagonal = (1 - chip) * 2 + (1 - core)

    def piece(w, owner, t):
        rows = mine[w].shape[1]
        return g[w].at[0, t // SUM_PIECES[w], pl.ds((owner * SUM_PIECES[w] + t % SUM_PIECES[w]) * rows, rows)]

    def place(ref, w, t):
        rows = mine[w].shape[1]
        return ref.at[t // SUM_PIECES[w], pl.ds((t % SUM_PIECES[w]) * rows, rows)]

    def to_partner(w, t):
        sems = in_send[w].at[t], in_recv[w].at[t]
        return pltpu.make_async_remote_copy(
            piece(w, diagonal, t), landed[w].at[t], *sems, device_id=(rep, partner), device_id_type=MESH
        )

    def to_mine(w, t):
        return pltpu.make_async_copy(piece(w, across, t), mine[w].at[t], load[w].at[t])

    def send_across(t):
        return pltpu.make_async_remote_copy(
            mine[0].at[t], place(across0, 0, t), out_send.at[t], out_recv.at[t], device_id=(rep, across), device_id_type=MESH
        )

    def keep(w, t):
        return pltpu.make_async_copy(mine[w].at[t], place(sums[w], w, t), store.at[w - 1, t])

    def own_terms(w):
        rows = theirs[w].shape[1]
        return pltpu.make_async_remote_copy(
            g[w].at[0, :, pl.ds(partner * rows, rows)], theirs[w], own_send.at[w], own_recv.at[w], device_id=(rep, partner), device_id_type=MESH
        )

    def add(w, t):
        to_partner(w, t).wait_recv()
        to_mine(w, t).wait()
        mine[w][t] = (mine[w][t].astype(F32) + landed[w][t].astype(F32)).astype(BF16)

    def each(w, body):
        pl.loop(0, 2 * SUM_PIECES[w])(body)

    barrier = pltpu.get_barrier_semaphore()
    for other in (partner, across):
        pl.semaphore_signal(barrier, inc=1, device_id=(rep, other), device_id_type=MESH)
    each(0, lambda t: to_mine(0, t).start())
    pl.semaphore_wait(barrier, 2)
    each(0, lambda t: to_partner(0, t).start())

    @pl.loop(0, 2 * SUM_PIECES[0])
    def _(t):
        add(0, t)

        @pl.when(core == 1)
        def _():
            send_across(t).start()

        @pl.when((core == 0) & (t >= LATE))
        def _():
            send_across(t - LATE).start()

    @pl.when(core == 0)
    def _():
        pl.loop(2 * SUM_PIECES[0] - LATE, 2 * SUM_PIECES[0])(lambda t: send_across(t).start())

    for w in (1, 2):

        @pl.loop(0, 2 * SUM_PIECES[w])
        def _(t, w=w):
            to_partner(w, t).start()
            to_mine(w, t).start()

    for w in range(3):
        own_terms(w).start()

    for w in (1, 2):

        @pl.loop(0, 2 * SUM_PIECES[w])
        def _(t, w=w):
            add(w, t)
            keep(w, t).start()

    for w in range(3):
        each(w, lambda t, w=w: to_partner(w, t).wait_send())
    for w in (1, 2):
        each(w, lambda t, w=w: keep(w, t).wait())
    for w in range(3):
        own_terms(w).wait()
    each(0, lambda t: send_across(t).wait())


def exchange(terms, blocks):
    shapes = [(2, *b) for b in blocks]
    vmem = [pltpu.VMEM((2 * n, b[0] // n, b[1]), BF16) for n, b in zip(SUM_PIECES, blocks, strict=True)]
    dma = pltpu.SemaphoreType.DMA
    sems = [dma((2 * n,)) for n in SUM_PIECES]
    return pl.pallas_call(
        pair_sums,
        out_shape=[jax.ShapeDtypeStruct(s, BF16) for s in (shapes[0], *shapes, *shapes[1:])],
        in_specs=[ANY] * 3,
        out_specs=[ANY] * 6,
        scratch_shapes=[
            *vmem,
            *vmem,
            *sems,
            *sems,
            *sems,
            sems[0],
            sems[0],
            dma((2, 2 * max(SUM_PIECES[1:]))),
            dma((3,)),
            dma((3,)),
        ],
        compiler_params=pltpu.CompilerParams(collective_id=0, has_side_effects=True, vmem_limit_bytes=60 << 20),
        cost_estimate=pl.CostEstimate(flops=10**8, bytes_accessed=10**8, transcendentals=0),
        name="pair_sums",
    )(*terms)


def adamw(per, splits, where, g, theirs, arrived, m, v, w):
    layers, block, columns = m.shape
    rows = block // per
    steps = layers * per
    firsts = [first // rows for first, _ in splits]
    counts = [size // rows for _, size in splits]

    def body(where_ref, g_ref, theirs_ref, arrived_ref, m_ref, v_ref, w_ref, m_out, v_out, w_out, *parts):
        total = (g_ref[0, 0].astype(F32) + theirs_ref[0].astype(F32)) + arrived_ref[0].astype(F32)
        grad = total.astype(BF16).astype(F32)
        old = w_ref[0].astype(F32)
        new_m = 0.9 * m_ref[0] + 0.1 * grad
        new_v = 0.95 * v_ref[0] + 0.05 * grad * grad
        step = new_m * lax.rsqrt(new_v + 1e-8) + 0.1 * old
        new_w = (old - 0.02 * step).astype(BF16)
        m_out[0] = new_m
        v_out[0] = new_v
        w_out[0] = new_w
        i = pl.program_id(0)
        for part, first, count in zip(parts, firsts, counts, strict=True):

            @pl.when((i >= first) & (i < first + count))
            def _(part=part):
                part[...] = new_w

    def own(i, where):
        return (i // per, i % per, 0)

    def inside(i, where):
        return (i // per, where[0] * per + i % per, 0)

    def part_map(first, count):
        return lambda i, where: (jnp.clip(i - first, 0, count - 1), 0)

    tile = (1, rows, columns)
    return pl.pallas_call(
        body,
        grid_spec=pltpu.PrefetchScalarGridSpec(
            num_scalar_prefetch=1,
            grid=(steps,),
            in_specs=[
                pl.BlockSpec((1, *tile), lambda i, where: (0, *inside(i, where))),
                pl.BlockSpec(tile, own),
                pl.BlockSpec(tile, own),
                pl.BlockSpec(tile, own),
                pl.BlockSpec(tile, own),
                pl.BlockSpec(tile, inside),
            ],
            out_specs=[
                pl.BlockSpec(tile, own),
                pl.BlockSpec(tile, own),
                pl.BlockSpec(tile, inside),
                *(pl.BlockSpec((rows, columns), part_map(f, c)) for f, c in zip(firsts, counts, strict=True)),
            ],
        ),
        out_shape=[
            jax.ShapeDtypeStruct(m.shape, F32),
            jax.ShapeDtypeStruct(m.shape, F32),
            jax.ShapeDtypeStruct(w.shape, BF16),
            *(jax.ShapeDtypeStruct((size, columns), BF16) for _, size in splits),
        ],
        cost_estimate=pl.CostEstimate(flops=10**10, bytes_accessed=10**8, transcendentals=0),
        name="adamw",
    )(where, g, theirs, arrived, m, v, w)


def put(per, where, whole, after, block, first, arrived):
    columns = whole.shape[2]
    rows = block // per
    count = min(a.shape[0] for _, _, a in arrived) // rows
    n = len(arrived)

    def body(where_ref, *refs):
        out = refs[-1]
        j = pl.program_id(1)
        for k in range(n):

            @pl.when(j == k)
            def _(k=k):
                out[0] = refs[k][...]

    def in_map(skip):
        return lambda i, j, where: (i + skip // rows, 0)

    def out_map(i, j, where):
        t = i + first // rows
        owner = where[arrived[0][0]]
        for k in range(1, n):
            owner = jnp.where(j == k, where[arrived[k][0]], owner)
        return (t // per, owner * per + t % per, 0)

    return pl.pallas_call(
        body,
        grid_spec=pltpu.PrefetchScalarGridSpec(
            num_scalar_prefetch=1,
            grid=(count, n),
            in_specs=[*(pl.BlockSpec((rows, columns), in_map(skip)) for _, skip, _ in arrived), HBM, HBM],
            out_specs=pl.BlockSpec((1, rows, columns), out_map),
        ),
        out_shape=jax.ShapeDtypeStruct(whole.shape, BF16),
        input_output_aliases={n + 1: 0},
        compiler_params=pltpu.CompilerParams(vmem_limit_bytes=16 << 20),
        cost_estimate=pl.CostEstimate(flops=10**9, bytes_accessed=10**7, transcendentals=0),
        name="put",
    )(where, *(a for _, _, a in arrived), whole, after)


def put_now(whole, block, first, arrived):
    layer, row = first // block, first % block
    size = arrived[0][1].shape[0]
    n = len(arrived)

    def body(*refs):
        out, sems = refs[-2:]
        me = lax.axis_index("dp")
        chip, core = me // 2, me % 2
        copies = []
        for k, (which, _) in enumerate(arrived):
            owner = (1 - chip if which // 2 else chip) * 2 + (1 - core if which % 2 else core)
            copies.append(pltpu.make_async_copy(refs[k], out.at[layer, pl.ds(owner * block + row, size)], sems.at[k]))
        for copy in copies:
            copy.start()
        for copy in copies:
            copy.wait()

    return pl.pallas_call(
        body,
        in_specs=[*(pl.BlockSpec(memory_space=pltpu.VMEM) for _ in range(n)), HBM],
        out_specs=HBM,
        out_shape=jax.ShapeDtypeStruct(whole.shape, BF16),
        scratch_shapes=[pltpu.SemaphoreType.DMA((n,))],
        input_output_aliases={n: 0},
        compiler_params=pltpu.CompilerParams(vmem_limit_bytes=16 << 20),
        cost_estimate=pl.CostEstimate(flops=10**9, bytes_accessed=10**7, transcendentals=0),
        name="put_now",
    )(*(a for _, a in arrived), whole)


def send(array, pairs):
    return lax.ppermute(array, "dp", pairs)


LAST = (12, 6, 3, 2, 1)


def solution(mesh):
    def step(*arrays):
        terms, weights, ms, vs = (arrays[i : i + 3] for i in (0, 3, 6, 9))
        blocks = [m.shape[1:] for m in ms]
        where = lax.axis_index("dp") ^ jnp.arange(4, dtype=jnp.int32)
        across0, theirs0, theirs1, theirs2, sum1, sum2 = exchange(terms, blocks)
        arrived = [across0, send(sum1, ACROSS), send(sum2, ACROSS)]
        theirs = [theirs0, theirs1, theirs2]
        new_w, new_m, new_v = [], [], []
        after = where
        for k in range(3):
            block = blocks[k][0]
            per = STEP_PIECES[k]
            rows = block // per
            splits = [(0, 2 * block)]
            if k == 2:
                splits += [(sum(LAST[:i]) * rows, LAST[i] * rows) for i in range(len(LAST))]
            m, v, w, block_w, *parts = adamw(per, splits, where, terms[k], theirs[k], arrived[k], ms[k], vs[k], weights[k])
            parts = parts or [block_w]
            over = [send(a, ACROSS) for a in parts]
            beside = send(block_w, PARTNER)
            passed = [send(a, PARTNER) for a in over]
            if k == 2:
                w = put(per, where, w, new_w[0], block, 0, [(1, 0, beside)])
            first = 0
            for i, (a, b) in enumerate(zip(over, passed, strict=True)):
                if k < 2:
                    w = put(per, where, w, after, block, first, [(1, first, beside), (2, 0, a), (3, 0, b)])
                elif LAST[i] > 3:
                    w = put(per, where, w, after, block, first, [(2, 0, a), (3, 0, b)])
                else:
                    w = put_now(w, block, first, [(2, a), (3, b)])
                first += a.shape[0]
            after = w
            new_w.append(w)
            new_m.append(m)
            new_v.append(v)
        return (*new_w, *new_m, *new_v)

    all_of, cut = P(None, None, None), P(None, "dp", None)
    return jax.shard_map(
        step,
        mesh=mesh,
        in_specs=(P(("rep", "dp"), None, None, None),) * 3 + (all_of,) * 3 + (cut,) * 6,
        out_specs=(P("rep", None, None),) * 3 + (P("rep", "dp", None),) * 6,
        check_vma=False,
    )
```

```python
import jax
import jax.numpy as jnp
from jax import lax
from jax.experimental import pallas as pl
from jax.experimental.pallas import tpu as pltpu
from jax.sharding import PartitionSpec as P


MESH = pl.DeviceIdType.MESH
BF16, F32 = jnp.bfloat16, jnp.float32
ANY = pl.BlockSpec(memory_space=pl.ANY)
HBM = pl.BlockSpec(memory_space=pltpu.HBM)
SUM_PIECES = (9, 6, 6)
STEP_PIECES = 3
STRIP = 16 * 4608
LATE = 12


PARTNER = [(i, i ^ 1) for i in range(4)]
ACROSS = [(i, i ^ 2) for i in range(4)]


def pair_sums(*refs):
    g = refs[0:3]
    across0 = refs[3]
    theirs = refs[4:7]
    sums = (None, *refs[7:9])
    mine, landed = refs[9:12], refs[12:15]
    in_send, in_recv, load = refs[15:18], refs[18:21], refs[21:24]
    out_send, out_recv, store, own_send, own_recv = refs[24:]

    rep, me = lax.axis_index("rep"), lax.axis_index("dp")
    chip, core = me // 2, me % 2
    partner = chip * 2 + (1 - core)
    across = (1 - chip) * 2 + core
    diagonal = (1 - chip) * 2 + (1 - core)

    def piece(w, owner, t):
        rows = mine[w].shape[1]
        return g[w].at[0, t // SUM_PIECES[w], pl.ds((owner * SUM_PIECES[w] + t % SUM_PIECES[w]) * rows, rows)]

    def place(ref, w, t):
        rows = mine[w].shape[1]
        return ref.at[t // SUM_PIECES[w], pl.ds((t % SUM_PIECES[w]) * rows, rows)]

    def to_partner(w, t):
        sems = in_send[w].at[t], in_recv[w].at[t]
        return pltpu.make_async_remote_copy(
            piece(w, diagonal, t), landed[w].at[t], *sems, device_id=(rep, partner), device_id_type=MESH
        )

    def to_mine(w, t):
        return pltpu.make_async_copy(piece(w, across, t), mine[w].at[t], load[w].at[t])

    def send_across(t):
        return pltpu.make_async_remote_copy(
            mine[0].at[t], place(across0, 0, t), out_send.at[t], out_recv.at[t], device_id=(rep, across), device_id_type=MESH
        )

    def keep(w, t):
        return pltpu.make_async_copy(mine[w].at[t], place(sums[w], w, t), store.at[w - 1, t])

    def own_terms(w):
        rows = theirs[w].shape[1]
        return pltpu.make_async_remote_copy(
            g[w].at[0, :, pl.ds(partner * rows, rows)], theirs[w], own_send.at[w], own_recv.at[w], device_id=(rep, partner), device_id_type=MESH
        )

    def add(w, t):
        to_partner(w, t).wait_recv()
        to_mine(w, t).wait()
        mine[w][t] = (mine[w][t].astype(F32) + landed[w][t].astype(F32)).astype(BF16)

    def each(w, body):
        pl.loop(0, 2 * SUM_PIECES[w])(body)

    barrier = pltpu.get_barrier_semaphore()
    for other in (partner, across):
        pl.semaphore_signal(barrier, inc=1, device_id=(rep, other), device_id_type=MESH)
    each(0, lambda t: to_mine(0, t).start())
    pl.semaphore_wait(barrier, 2)
    each(0, lambda t: to_partner(0, t).start())

    @pl.loop(0, 2 * SUM_PIECES[0])
    def _(t):
        add(0, t)

        @pl.when(core == 1)
        def _():
            send_across(t).start()

        @pl.when((core == 0) & (t >= LATE))
        def _():
            send_across(t - LATE).start()

    @pl.when(core == 0)
    def _():
        pl.loop(2 * SUM_PIECES[0] - LATE, 2 * SUM_PIECES[0])(lambda t: send_across(t).start())

    for w in (1, 2):

        @pl.loop(0, 2 * SUM_PIECES[w])
        def _(t, w=w):
            to_partner(w, t).start()
            to_mine(w, t).start()

    for w in range(3):
        own_terms(w).start()

    for w in (1, 2):

        @pl.loop(0, 2 * SUM_PIECES[w])
        def _(t, w=w):
            add(w, t)
            keep(w, t).start()

    for w in range(3):
        each(w, lambda t, w=w: to_partner(w, t).wait_send())
    for w in (1, 2):
        each(w, lambda t, w=w: keep(w, t).wait())
    for w in range(3):
        own_terms(w).wait()
    each(0, lambda t: send_across(t).wait())


def exchange(terms, blocks):
    shapes = [(2, *b) for b in blocks]
    vmem = [pltpu.VMEM((2 * n, b[0] // n, b[1]), BF16) for n, b in zip(SUM_PIECES, blocks, strict=True)]
    dma = pltpu.SemaphoreType.DMA
    sems = [dma((2 * n,)) for n in SUM_PIECES]
    return pl.pallas_call(
        pair_sums,
        out_shape=[jax.ShapeDtypeStruct(s, BF16) for s in (shapes[0], *shapes, *shapes[1:])],
        in_specs=[ANY] * 3,
        out_specs=[ANY] * 6,
        scratch_shapes=[
            *vmem,
            *vmem,
            *sems,
            *sems,
            *sems,
            sems[0],
            sems[0],
            dma((2, 2 * max(SUM_PIECES[1:]))),
            dma((3,)),
            dma((3,)),
        ],
        compiler_params=pltpu.CompilerParams(collective_id=0, has_side_effects=True, vmem_limit_bytes=60 << 20),
        cost_estimate=pl.CostEstimate(flops=10**8, bytes_accessed=10**8, transcendentals=0),
        name="pair_sums",
    )(*terms)


def adamw(splits, where, g, theirs, arrived, m, v, w):
    layers, block, columns = m.shape
    rows = block // STEP_PIECES
    strip = STRIP // columns
    steps = layers * STEP_PIECES

    def body(where_ref, g_ref, theirs_ref, arrived_ref, m_ref, v_ref, w_ref, m_out, v_out, w_out, *parts):
        @pl.loop(0, rows // strip)
        def _(j):
            at = pl.ds(pl.multiple_of(j * strip, strip), strip)
            total = (g_ref[0, 0, at].astype(F32) + theirs_ref[0, at].astype(F32)) + arrived_ref[0, at].astype(F32)
            grad = total.astype(BF16).astype(F32)
            old = w_ref[0, at].astype(F32)
            new_m = 0.9 * m_ref[0, at] + 0.1 * grad
            new_v = 0.95 * v_ref[0, at] + 0.05 * grad * grad
            step = new_m * lax.rsqrt(new_v + 1e-8) + 0.1 * old
            m_out[0, at] = new_m
            v_out[0, at] = new_v
            w_out[0, at] = (old - 0.02 * step).astype(BF16)

        i = pl.program_id(0)
        for part, (first, size) in zip(parts, splits, strict=True):
            for n in range(steps):
                low, high = max(first, n * rows), min(first + size, (n + 1) * rows)
                if low < high:

                    @pl.when(i == n)
                    def _(part=part, first=first, low=low, high=high, n=n):
                        part[low - first : high - first] = w_out[0, low - n * rows : high - n * rows]

    def own(i, where):
        return (i // STEP_PIECES, i % STEP_PIECES, 0)

    def inside(i, where):
        return (i // STEP_PIECES, where[0] * STEP_PIECES + i % STEP_PIECES, 0)

    tile = (1, rows, columns)
    return pl.pallas_call(
        body,
        grid_spec=pltpu.PrefetchScalarGridSpec(
            num_scalar_prefetch=1,
            grid=(steps,),
            in_specs=[
                pl.BlockSpec((1, *tile), lambda i, where: (0, *inside(i, where))),
                pl.BlockSpec(tile, own),
                pl.BlockSpec(tile, own),
                pl.BlockSpec(tile, own),
                pl.BlockSpec(tile, own),
                pl.BlockSpec(tile, inside),
            ],
            out_specs=[
                pl.BlockSpec(tile, own),
                pl.BlockSpec(tile, own),
                pl.BlockSpec(tile, inside),
                *(pl.BlockSpec((size, columns), lambda i, where: (0, 0)) for _, size in splits),
            ],
        ),
        out_shape=[
            jax.ShapeDtypeStruct(m.shape, F32),
            jax.ShapeDtypeStruct(m.shape, F32),
            jax.ShapeDtypeStruct(w.shape, BF16),
            *(jax.ShapeDtypeStruct((size, columns), BF16) for _, size in splits),
        ],
        cost_estimate=pl.CostEstimate(flops=10**10, bytes_accessed=10**8, transcendentals=0),
        name="adamw",
    )(where, g, theirs, arrived, m, v, w)


def put(whole, block, arrived, after=()):
    n = len(arrived)
    moves = []
    for k, (which, first, array) in enumerate(arrived):
        for layer in range(2):
            low, high = max(first, layer * block), min(first + array.shape[0], (layer + 1) * block)
            if low < high:
                moves.append((k, which, layer, low - first, low - layer * block, high - low))

    def body(*refs):
        out, sems = refs[-2:]
        me = lax.axis_index("dp")
        chip, core = me // 2, me % 2

        def copy(j):
            k, which, layer, source, row, size = moves[j]
            owner = (1 - chip if which // 2 else chip) * 2 + (1 - core if which % 2 else core)
            return pltpu.make_async_copy(refs[k].at[pl.ds(source, size)], out.at[layer, pl.ds(owner * block + row, size)], sems.at[j])

        for j in range(len(moves)):
            copy(j).start()
        for j in range(len(moves)):
            copy(j).wait()

    return pl.pallas_call(
        body,
        in_specs=[*(pl.BlockSpec(memory_space=pltpu.VMEM) for _ in range(n)), HBM, *(HBM for _ in after)],
        out_specs=HBM,
        out_shape=jax.ShapeDtypeStruct(whole.shape, BF16),
        scratch_shapes=[pltpu.SemaphoreType.DMA((len(moves),))],
        input_output_aliases={n: 0},
        compiler_params=pltpu.CompilerParams(vmem_limit_bytes=20 << 20),
        cost_estimate=pl.CostEstimate(flops=10**9, bytes_accessed=10**7, transcendentals=0),
        name="put",
    )(*(a for *_, a in arrived), whole, *after)


def send(array, pairs):
    return lax.ppermute(array, "dp", pairs)


LAST = (1152, 576, 288, 192, 64, 32)


def solution(mesh):
    def step(*arrays):
        terms, weights, ms, vs = (arrays[i : i + 3] for i in (0, 3, 6, 9))
        blocks = [m.shape[1:] for m in ms]
        where = lax.axis_index("dp") ^ jnp.arange(4, dtype=jnp.int32)
        across0, theirs0, theirs1, theirs2, sum1, sum2 = exchange(terms, blocks)
        arrived = [across0, send(sum1, ACROSS), send(sum2, ACROSS)]
        theirs = [theirs0, theirs1, theirs2]
        new_w, new_m, new_v = [], [], []

        for k in range(3):
            block = blocks[k][0]
            splits = [(0, 2 * block)]
            if k == 2:
                splits += [(sum(LAST[:i]), LAST[i]) for i in range(len(LAST))]
            m, v, w, block_w, *parts = adamw(splits, where, terms[k], theirs[k], arrived[k], ms[k], vs[k], weights[k])
            beside = send(block_w, PARTNER)
            if k < 2:
                over = send(block_w, ACROSS)
                passed = send(over, PARTNER)
                w = put(w, block, [(1, 0, beside), (2, 0, over), (3, 0, passed)], new_w)
            else:
                w = put(w, block, [(1, 0, beside)], new_w[:1])
                over = [send(a, ACROSS) for a in parts]
                passed = [send(a, PARTNER) for a in over]
                for i in range(5):
                    last = (4, 5) if i == 4 else (i,)
                    pairs = [(which, splits[1 + j][0], a[j]) for j in last for which, a in ((2, over), (3, passed))]
                    w = put(w, block, pairs, new_w if i == 0 else ())
            new_w.append(w)
            new_m.append(m)
            new_v.append(v)
        return (*new_w, *new_m, *new_v)

    all_of, cut = P(None, None, None), P(None, "dp", None)
    return jax.shard_map(
        step,
        mesh=mesh,
        in_specs=(P(("rep", "dp"), None, None, None),) * 3 + (all_of,) * 3 + (cut,) * 6,
        out_specs=(P("rep", None, None),) * 3 + (P("rep", "dp", None),) * 6,
        check_vma=False,
    )
```

```python
import jax
import jax.numpy as jnp
from jax import lax
from jax.experimental import pallas as pl
from jax.experimental.pallas import tpu as pltpu
from jax.sharding import PartitionSpec as P


MESH = pl.DeviceIdType.MESH
BF16, F32 = jnp.bfloat16, jnp.float32
ANY = pl.BlockSpec(memory_space=pl.ANY)
HBM = pl.BlockSpec(memory_space=pltpu.HBM)
SUM_PIECES = (18, 6, 6)
STEP_PIECES = 3
STRIP = 16 * 4608
LATE = 32


PARTNER = [(i, i ^ 1) for i in range(4)]
ACROSS = [(i, i ^ 2) for i in range(4)]


def pair_sums(*refs):
    g = refs[0:3]
    across0 = refs[3]
    theirs = refs[4:7]
    sums = (None, *refs[7:9])
    mine, landed = refs[9:12], refs[12:15]
    in_send, in_recv, load = refs[15:18], refs[18:21], refs[21:24]
    out_send, out_recv, store, own_send, own_recv = refs[24:]

    rep, me = lax.axis_index("rep"), lax.axis_index("dp")
    chip, core = me // 2, me % 2
    partner = chip * 2 + (1 - core)
    across = (1 - chip) * 2 + core
    diagonal = (1 - chip) * 2 + (1 - core)

    def piece(w, owner, t):
        rows = mine[w].shape[1]
        return g[w].at[0, t // SUM_PIECES[w], pl.ds((owner * SUM_PIECES[w] + t % SUM_PIECES[w]) * rows, rows)]

    def place(ref, w, t):
        rows = mine[w].shape[1]
        return ref.at[t // SUM_PIECES[w], pl.ds((t % SUM_PIECES[w]) * rows, rows)]

    def to_partner(w, t):
        sems = in_send[w].at[t], in_recv[w].at[t]
        return pltpu.make_async_remote_copy(
            piece(w, diagonal, t), landed[w].at[t], *sems, device_id=(rep, partner), device_id_type=MESH
        )

    def to_mine(w, t):
        return pltpu.make_async_copy(piece(w, across, t), mine[w].at[t], load[w].at[t])

    def send_across(t):
        return pltpu.make_async_remote_copy(
            mine[0].at[t], place(across0, 0, t), out_send.at[t], out_recv.at[t], device_id=(rep, across), device_id_type=MESH
        )

    def keep(w, t):
        return pltpu.make_async_copy(mine[w].at[t], place(sums[w], w, t), store.at[w - 1, t])

    def own_terms(w):
        rows = theirs[w].shape[1]
        return pltpu.make_async_remote_copy(
            g[w].at[0, :, pl.ds(partner * rows, rows)], theirs[w], own_send.at[w], own_recv.at[w], device_id=(rep, partner), device_id_type=MESH
        )

    def add(w, t):
        to_partner(w, t).wait_recv()
        to_mine(w, t).wait()
        mine[w][t] = (mine[w][t].astype(F32) + landed[w][t].astype(F32)).astype(BF16)

    def each(w, body):
        pl.loop(0, 2 * SUM_PIECES[w])(body)

    barrier = pltpu.get_barrier_semaphore()
    for other in (partner, across):
        pl.semaphore_signal(barrier, inc=1, device_id=(rep, other), device_id_type=MESH)
    each(0, lambda t: to_mine(0, t).start())
    pl.semaphore_wait(barrier, 2)
    each(0, lambda t: to_partner(0, t).start())

    @pl.loop(0, 2 * SUM_PIECES[0])
    def _(t):
        add(0, t)

        @pl.when(core == 0)
        def _():
            send_across(t).start()

        @pl.when((core == 1) & (t >= LATE))
        def _():
            send_across(t - LATE).start()

    @pl.when(core == 1)
    def _():
        pl.loop(2 * SUM_PIECES[0] - LATE, 2 * SUM_PIECES[0])(lambda t: send_across(t).start())

    for w in (1, 2):

        @pl.loop(0, 2 * SUM_PIECES[w])
        def _(t, w=w):
            to_partner(w, t).start()
            to_mine(w, t).start()

    for w in range(3):
        own_terms(w).start()

    for w in (1, 2):

        @pl.loop(0, 2 * SUM_PIECES[w])
        def _(t, w=w):
            add(w, t)
            keep(w, t).start()

    for w in range(3):
        each(w, lambda t, w=w: to_partner(w, t).wait_send())
    for w in (1, 2):
        each(w, lambda t, w=w: keep(w, t).wait())
    for w in range(3):
        own_terms(w).wait()
    each(0, lambda t: send_across(t).wait())


def exchange(terms, blocks):
    shapes = [(2, *b) for b in blocks]
    vmem = [pltpu.VMEM((2 * n, b[0] // n, b[1]), BF16) for n, b in zip(SUM_PIECES, blocks, strict=True)]
    dma = pltpu.SemaphoreType.DMA
    sems = [dma((2 * n,)) for n in SUM_PIECES]
    return pl.pallas_call(
        pair_sums,
        out_shape=[jax.ShapeDtypeStruct(s, BF16) for s in (shapes[0], *shapes, *shapes[1:])],
        in_specs=[ANY] * 3,
        out_specs=[ANY] * 6,
        scratch_shapes=[
            *vmem,
            *vmem,
            *sems,
            *sems,
            *sems,
            sems[0],
            sems[0],
            dma((2, 2 * max(SUM_PIECES[1:]))),
            dma((3,)),
            dma((3,)),
        ],
        compiler_params=pltpu.CompilerParams(collective_id=0, has_side_effects=True, vmem_limit_bytes=60 << 20),
        cost_estimate=pl.CostEstimate(flops=10**8, bytes_accessed=10**8, transcendentals=0),
        name="pair_sums",
    )(*terms)


def adamw(splits, where, g, theirs, arrived, m, v, w):
    layers, block, columns = m.shape
    rows = block // STEP_PIECES
    strip = STRIP // columns
    steps = layers * STEP_PIECES

    def body(where_ref, g_ref, theirs_ref, arrived_ref, m_ref, v_ref, w_ref, m_out, v_out, w_out, *parts):
        @pl.loop(0, rows // strip)
        def _(j):
            at = pl.ds(pl.multiple_of(j * strip, strip), strip)
            total = (g_ref[0, 0, at].astype(F32) + theirs_ref[0, at].astype(F32)) + arrived_ref[0, at].astype(F32)
            grad = total.astype(BF16).astype(F32)
            old = w_ref[0, at].astype(F32)
            new_m = 0.9 * m_ref[0, at] + 0.1 * grad
            new_v = 0.95 * v_ref[0, at] + 0.05 * grad * grad
            step = new_m * lax.rsqrt(new_v + 1e-8) + 0.1 * old
            m_out[0, at] = new_m
            v_out[0, at] = new_v
            w_out[0, at] = (old - 0.02 * step).astype(BF16)

        i = pl.program_id(0)
        for part, (first, size) in zip(parts, splits, strict=True):
            for n in range(steps):
                low, high = max(first, n * rows), min(first + size, (n + 1) * rows)
                if low < high:

                    @pl.when(i == n)
                    def _(part=part, first=first, low=low, high=high, n=n):
                        part[low - first : high - first] = w_out[0, low - n * rows : high - n * rows]

    def own(i, where):
        return (i // STEP_PIECES, i % STEP_PIECES, 0)

    def inside(i, where):
        return (i // STEP_PIECES, where[0] * STEP_PIECES + i % STEP_PIECES, 0)

    tile = (1, rows, columns)
    return pl.pallas_call(
        body,
        grid_spec=pltpu.PrefetchScalarGridSpec(
            num_scalar_prefetch=1,
            grid=(steps,),
            in_specs=[
                pl.BlockSpec((1, *tile), lambda i, where: (0, *inside(i, where))),
                pl.BlockSpec(tile, own),
                pl.BlockSpec(tile, own),
                pl.BlockSpec(tile, own),
                pl.BlockSpec(tile, own),
                pl.BlockSpec(tile, inside),
            ],
            out_specs=[
                pl.BlockSpec(tile, own),
                pl.BlockSpec(tile, own),
                pl.BlockSpec(tile, inside),
                *(pl.BlockSpec((size, columns), lambda i, where: (0, 0)) for _, size in splits),
            ],
        ),
        out_shape=[
            jax.ShapeDtypeStruct(m.shape, F32),
            jax.ShapeDtypeStruct(m.shape, F32),
            jax.ShapeDtypeStruct(w.shape, BF16),
            *(jax.ShapeDtypeStruct((size, columns), BF16) for _, size in splits),
        ],
        cost_estimate=pl.CostEstimate(flops=10**10, bytes_accessed=10**8, transcendentals=0),
        name="adamw",
    )(where, g, theirs, arrived, m, v, w)


def put(whole, block, arrived, after=()):
    n = len(arrived)
    moves = []
    for k, (which, first, array) in enumerate(arrived):
        for layer in range(2):
            low, high = max(first, layer * block), min(first + array.shape[0], (layer + 1) * block)
            if low < high:
                moves.append((k, which, layer, low - first, low - layer * block, high - low))

    def body(*refs):
        out, sems = refs[-2:]
        me = lax.axis_index("dp")
        chip, core = me // 2, me % 2

        def copy(j):
            k, which, layer, source, row, size = moves[j]
            owner = (1 - chip if which // 2 else chip) * 2 + (1 - core if which % 2 else core)
            return pltpu.make_async_copy(refs[k].at[pl.ds(source, size)], out.at[layer, pl.ds(owner * block + row, size)], sems.at[j])

        for j in range(len(moves)):
            copy(j).start()
        for j in range(len(moves)):
            copy(j).wait()

    return pl.pallas_call(
        body,
        in_specs=[*(pl.BlockSpec(memory_space=pltpu.VMEM) for _ in range(n)), HBM, *(HBM for _ in after)],
        out_specs=HBM,
        out_shape=jax.ShapeDtypeStruct(whole.shape, BF16),
        scratch_shapes=[pltpu.SemaphoreType.DMA((len(moves),))],
        input_output_aliases={n: 0},
        compiler_params=pltpu.CompilerParams(vmem_limit_bytes=20 << 20),
        cost_estimate=pl.CostEstimate(flops=10**9, bytes_accessed=10**7, transcendentals=0),
        name="put",
    )(*(a for *_, a in arrived), whole, *after)


def send(array, pairs):
    return lax.ppermute(array, "dp", pairs)


LAST = (1152, 576, 288, 192, 64, 32)


def solution(mesh):
    def step(*arrays):
        terms, weights, ms, vs = (arrays[i : i + 3] for i in (0, 3, 6, 9))
        blocks = [m.shape[1:] for m in ms]
        where = lax.axis_index("dp") ^ jnp.arange(4, dtype=jnp.int32)
        across0, theirs0, theirs1, theirs2, sum1, sum2 = exchange(terms, blocks)
        arrived = [across0, send(sum1, ACROSS), send(sum2, ACROSS)]
        theirs = [theirs0, theirs1, theirs2]
        new_w, new_m, new_v = [], [], []

        for k in range(3):
            block = blocks[k][0]
            splits = [(0, 2 * block)]
            if k == 2:
                splits += [(sum(LAST[:i]), LAST[i]) for i in range(len(LAST))]
            m, v, w, block_w, *parts = adamw(splits, where, terms[k], theirs[k], arrived[k], ms[k], vs[k], weights[k])
            beside = send(block_w, PARTNER)
            if k < 2:
                over = send(block_w, ACROSS)
                passed = send(over, PARTNER)
                w = put(w, block, [(1, 0, beside), (2, 0, over), (3, 0, passed)], new_w)
            else:
                w = put(w, block, [(1, 0, beside)], new_w[:1])
                over = [send(a, ACROSS) for a in parts]
                passed = [send(a, PARTNER) for a in over]
                for i in range(5):
                    last = (4, 5) if i == 4 else (i,)
                    pairs = [(which, splits[1 + j][0], a[j]) for j in last for which, a in ((2, over), (3, passed))]
                    w = put(w, block, pairs, new_w if i == 0 else ())
            new_w.append(w)
            new_m.append(m)
            new_v.append(v)
        return (*new_w, *new_m, *new_v)

    all_of, cut = P(None, None, None), P(None, "dp", None)
    return jax.shard_map(
        step,
        mesh=mesh,
        in_specs=(P(("rep", "dp"), None, None, None),) * 3 + (all_of,) * 3 + (cut,) * 6,
        out_specs=(P("rep", None, None),) * 3 + (P("rep", "dp", None),) * 6,
        check_vma=False,
    )
```

```python
import jax
import jax.numpy as jnp
from jax import lax
from jax.experimental import pallas as pl
from jax.experimental.pallas import tpu as pltpu
from jax.sharding import PartitionSpec as P


MESH = pl.DeviceIdType.MESH
BF16, F32 = jnp.bfloat16, jnp.float32
ANY = pl.BlockSpec(memory_space=pl.ANY)
HBM = pl.BlockSpec(memory_space=pltpu.HBM)
SUM_PIECES = (18, 6, 6)
STEP_PIECES = 3
STRIP = 16 * 4608
LATE = 32


PARTNER = [(i, i ^ 1) for i in range(4)]
ACROSS = [(i, i ^ 2) for i in range(4)]


def pair_sums(*refs):
    g = refs[0:3]
    across0 = refs[3]
    theirs = refs[4:7]
    sums = (None, *refs[7:9])
    mine, landed = refs[9:12], refs[12:15]
    in_send, in_recv, load = refs[15:18], refs[18:21], refs[21:24]
    out_send, out_recv, store, own_send, own_recv = refs[24:]

    rep, me = lax.axis_index("rep"), lax.axis_index("dp")
    chip, core = me // 2, me % 2
    partner = chip * 2 + (1 - core)
    across = (1 - chip) * 2 + core
    diagonal = (1 - chip) * 2 + (1 - core)

    def piece(w, owner, t):
        rows = mine[w].shape[1]
        return g[w].at[0, t // SUM_PIECES[w], pl.ds((owner * SUM_PIECES[w] + t % SUM_PIECES[w]) * rows, rows)]

    def place(ref, w, t):
        rows = mine[w].shape[1]
        return ref.at[t // SUM_PIECES[w], pl.ds((t % SUM_PIECES[w]) * rows, rows)]

    def to_partner(w, t):
        sems = in_send[w].at[t], in_recv[w].at[t]
        return pltpu.make_async_remote_copy(
            piece(w, diagonal, t), landed[w].at[t], *sems, device_id=(rep, partner), device_id_type=MESH
        )

    def to_mine(w, t):
        return pltpu.make_async_copy(piece(w, across, t), mine[w].at[t], load[w].at[t])

    def send_across(t):
        return pltpu.make_async_remote_copy(
            mine[0].at[t], place(across0, 0, t), out_send.at[t], out_recv.at[t], device_id=(rep, across), device_id_type=MESH
        )

    def keep(w, t):
        return pltpu.make_async_copy(mine[w].at[t], place(sums[w], w, t), store.at[w - 1, t])

    def own_terms(w):
        rows = theirs[w].shape[1]
        return pltpu.make_async_remote_copy(
            g[w].at[0, :, pl.ds(partner * rows, rows)], theirs[w], own_send.at[w], own_recv.at[w], device_id=(rep, partner), device_id_type=MESH
        )

    def add(w, t):
        to_partner(w, t).wait_recv()
        to_mine(w, t).wait()
        mine[w][t] = (mine[w][t].astype(F32) + landed[w][t].astype(F32)).astype(BF16)

    def each(w, body):
        pl.loop(0, 2 * SUM_PIECES[w])(body)

    barrier = pltpu.get_barrier_semaphore()
    for other in (partner, across):
        pl.semaphore_signal(barrier, inc=1, device_id=(rep, other), device_id_type=MESH)
    each(0, lambda t: to_mine(0, t).start())
    pl.semaphore_wait(barrier, 2)
    each(0, lambda t: to_partner(0, t).start())

    @pl.loop(0, 2 * SUM_PIECES[0])
    def _(t):
        add(0, t)

        @pl.when(core == 0)
        def _():
            send_across(t).start()

        @pl.when((core == 1) & (t >= LATE))
        def _():
            send_across(t - LATE).start()

    @pl.when(core == 1)
    def _():
        pl.loop(2 * SUM_PIECES[0] - LATE, 2 * SUM_PIECES[0])(lambda t: send_across(t).start())

    for w in (1, 2):

        @pl.loop(0, 2 * SUM_PIECES[w])
        def _(t, w=w):
            to_partner(w, t).start()
            to_mine(w, t).start()

    for w in range(3):
        own_terms(w).start()

    for w in (1, 2):

        @pl.loop(0, 2 * SUM_PIECES[w])
        def _(t, w=w):
            add(w, t)
            keep(w, t).start()

    for w in range(3):
        each(w, lambda t, w=w: to_partner(w, t).wait_send())
    for w in (1, 2):
        each(w, lambda t, w=w: keep(w, t).wait())
    for w in range(3):
        own_terms(w).wait()
    each(0, lambda t: send_across(t).wait())


def exchange(terms, blocks):
    shapes = [(2, *b) for b in blocks]
    vmem = [pltpu.VMEM((2 * n, b[0] // n, b[1]), BF16) for n, b in zip(SUM_PIECES, blocks, strict=True)]
    dma = pltpu.SemaphoreType.DMA
    sems = [dma((2 * n,)) for n in SUM_PIECES]
    return pl.pallas_call(
        pair_sums,
        out_shape=[jax.ShapeDtypeStruct(s, BF16) for s in (shapes[0], *shapes, *shapes[1:])],
        in_specs=[ANY] * 3,
        out_specs=[ANY] * 6,
        scratch_shapes=[
            *vmem,
            *vmem,
            *sems,
            *sems,
            *sems,
            sems[0],
            sems[0],
            dma((2, 2 * max(SUM_PIECES[1:]))),
            dma((3,)),
            dma((3,)),
        ],
        compiler_params=pltpu.CompilerParams(collective_id=0, has_side_effects=True, vmem_limit_bytes=60 << 20),
        cost_estimate=pl.CostEstimate(flops=10**8, bytes_accessed=10**8, transcendentals=0),
        name="pair_sums",
    )(*terms)


def adamw(splits, where, g, theirs, arrived, m, v, w):
    layers, block, columns = m.shape
    rows = block // STEP_PIECES
    strip = STRIP // columns
    steps = layers * STEP_PIECES

    def body(where_ref, g_ref, theirs_ref, arrived_ref, m_ref, v_ref, w_ref, m_out, v_out, w_out, *parts):
        @pl.loop(0, rows // strip)
        def _(j):
            at = pl.ds(pl.multiple_of(j * strip, strip), strip)
            total = (g_ref[0, 0, at].astype(F32) + theirs_ref[0, at].astype(F32)) + arrived_ref[0, at].astype(F32)
            grad = total.astype(BF16).astype(F32)
            old = w_ref[0, at].astype(F32)
            new_m = 0.9 * m_ref[0, at] + 0.1 * grad
            new_v = 0.95 * v_ref[0, at] + 0.05 * grad * grad
            step = new_m * lax.rsqrt(new_v + 1e-8) + 0.1 * old
            m_out[0, at] = new_m
            v_out[0, at] = new_v
            w_out[0, at] = (old - 0.02 * step).astype(BF16)

        i = pl.program_id(0)
        for part, (first, size) in zip(parts, splits, strict=True):
            for n in range(steps):
                low, high = max(first, n * rows), min(first + size, (n + 1) * rows)
                if low < high:

                    @pl.when(i == n)
                    def _(part=part, first=first, low=low, high=high, n=n):
                        part[low - first : high - first] = w_out[0, low - n * rows : high - n * rows]

    def own(i, where):
        return (i // STEP_PIECES, i % STEP_PIECES, 0)

    def inside(i, where):
        return (i // STEP_PIECES, where[0] * STEP_PIECES + i % STEP_PIECES, 0)

    tile = (1, rows, columns)
    return pl.pallas_call(
        body,
        grid_spec=pltpu.PrefetchScalarGridSpec(
            num_scalar_prefetch=1,
            grid=(steps,),
            in_specs=[
                pl.BlockSpec((1, *tile), lambda i, where: (0, *inside(i, where))),
                pl.BlockSpec(tile, own),
                pl.BlockSpec(tile, own),
                pl.BlockSpec(tile, own),
                pl.BlockSpec(tile, own),
                pl.BlockSpec(tile, inside),
            ],
            out_specs=[
                pl.BlockSpec(tile, own),
                pl.BlockSpec(tile, own),
                pl.BlockSpec(tile, inside),
                *(pl.BlockSpec((size, columns), lambda i, where: (0, 0)) for _, size in splits),
            ],
        ),
        out_shape=[
            jax.ShapeDtypeStruct(m.shape, F32),
            jax.ShapeDtypeStruct(m.shape, F32),
            jax.ShapeDtypeStruct(w.shape, BF16),
            *(jax.ShapeDtypeStruct((size, columns), BF16) for _, size in splits),
        ],
        cost_estimate=pl.CostEstimate(flops=10**10, bytes_accessed=10**8, transcendentals=0),
        name="adamw",
    )(where, g, theirs, arrived, m, v, w)


def put(whole, block, arrived, after=()):
    n = len(arrived)
    moves = []
    for k, (which, first, array) in enumerate(arrived):
        for layer in range(2):
            low, high = max(first, layer * block), min(first + array.shape[0], (layer + 1) * block)
            if low < high:
                moves.append((k, which, layer, low - first, low - layer * block, high - low))

    def body(*refs):
        out, sems = refs[-2:]
        me = lax.axis_index("dp")
        chip, core = me // 2, me % 2

        def copy(j):
            k, which, layer, source, row, size = moves[j]
            owner = (1 - chip if which // 2 else chip) * 2 + (1 - core if which % 2 else core)
            return pltpu.make_async_copy(refs[k].at[pl.ds(source, size)], out.at[layer, pl.ds(owner * block + row, size)], sems.at[j])

        for j in range(len(moves)):
            copy(j).start()
        for j in range(len(moves)):
            copy(j).wait()

    return pl.pallas_call(
        body,
        in_specs=[*(pl.BlockSpec(memory_space=pltpu.VMEM) for _ in range(n)), HBM, *(HBM for _ in after)],
        out_specs=HBM,
        out_shape=jax.ShapeDtypeStruct(whole.shape, BF16),
        scratch_shapes=[pltpu.SemaphoreType.DMA((len(moves),))],
        input_output_aliases={n: 0},
        compiler_params=pltpu.CompilerParams(vmem_limit_bytes=20 << 20),
        cost_estimate=pl.CostEstimate(flops=10**9, bytes_accessed=10**7, transcendentals=0),
        name="put",
    )(*(a for *_, a in arrived), whole, *after)


def send(array, pairs):
    return lax.ppermute(array, "dp", pairs)


LAST = (1152, 576, 368, 144, 48, 16)


def solution(mesh):
    def step(*arrays):
        terms, weights, ms, vs = (arrays[i : i + 3] for i in (0, 3, 6, 9))
        blocks = [m.shape[1:] for m in ms]
        where = lax.axis_index("dp") ^ jnp.arange(4, dtype=jnp.int32)
        across0, theirs0, theirs1, theirs2, sum1, sum2 = exchange(terms, blocks)
        arrived = [across0, send(sum1, ACROSS), send(sum2, ACROSS)]
        theirs = [theirs0, theirs1, theirs2]
        new_w, new_m, new_v = [], [], []

        for k in range(3):
            block = blocks[k][0]
            splits = [(0, 2 * block)]
            if k == 2:
                splits += [(sum(LAST[:i]), LAST[i]) for i in range(len(LAST))]
            m, v, w, block_w, *parts = adamw(splits, where, terms[k], theirs[k], arrived[k], ms[k], vs[k], weights[k])
            beside = send(block_w, PARTNER)
            if k < 2:
                over = send(block_w, ACROSS)
                passed = send(over, PARTNER)
                w = put(w, block, [(1, 0, beside), (2, 0, over), (3, 0, passed)], new_w)
            else:
                w = put(w, block, [(1, 0, beside)], new_w[:1])
                over = [send(a, ACROSS) for a in parts]
                passed = [send(a, PARTNER) for a in over]
                for i in range(5):
                    here, handed = ((i, i + 1, i + 2), (i,)) if i == 3 else ((), (4, 5)) if i == 4 else ((i,), (i,))
                    pairs = [(2, splits[1 + j][0], over[j]) for j in here] + [(3, splits[1 + j][0], passed[j]) for j in handed]
                    w = put(w, block, pairs, new_w if i == 0 else ())
            new_w.append(w)
            new_m.append(m)
            new_v.append(v)
        return (*new_w, *new_m, *new_v)

    all_of, cut = P(None, None, None), P(None, "dp", None)
    return jax.shard_map(
        step,
        mesh=mesh,
        in_specs=(P(("rep", "dp"), None, None, None),) * 3 + (all_of,) * 3 + (cut,) * 6,
        out_specs=(P("rep", None, None),) * 3 + (P("rep", "dp", None),) * 6,
        check_vma=False,
    )
```
